32 devices in a mesh: dp: 4 (over y, z), ep: 8 (over x, core).
Axes of the slice: x: 4, y: 2, z: 2, core: 2. Of those that a mesh axis runs over, the one named last changes fastest.
The devices are a block of a 4x4x8 slice.
Arguments:
- h0: bfloat16 [32, 512, 2048], P(('dp', 'ep')), parts along dimension 0
- idx: int32 [32, 512, 6], P(('dp', 'ep')), parts along dimension 0
- slot: int32 [32, 512, 6], P(('dp', 'ep')), parts along dimension 0
- ln_attn: bfloat16 [2048], replicated
- wq: bfloat16 [2048, 2048], replicated
- wk: bfloat16 [2048, 2048], replicated
- wv: bfloat16 [2048, 2048], replicated
- wo: bfloat16 [2048, 2048], replicated
- ln_ffn: bfloat16 [2048], replicated
- ws1: bfloat16 [2048, 2816], replicated
- ws3: bfloat16 [2048, 2816], replicated
- ws2: bfloat16 [2816, 2048], replicated
- ln_moe: bfloat16 [2048], replicated
- wr: bfloat16 [2048, 64], replicated
- ue1: bfloat16 [64, 2048, 1408], P('ep')
- ue3: bfloat16 [64, 2048, 1408], P('ep')
- ue2: bfloat16 [64, 1408, 2048], P('ep')
Outputs:
- output: bfloat16 [32, 512, 2048], P(('dp', 'ep')), parts along dimension 0
There are 4 independent parts. The reference program is written for one: setup_inputs(seed, part) draws one part's arguments, and reference() takes and returns one part's arrays. A program takes and returns all parts, laid end to end along the dimension named above; an argument that names none is the same for every part.
All inputs are finite; a program needn't handle non-finite values.
Results may differ from the reference program's by a relative error of at most 0.0103379.
Values are sent between devices in bfloat16 or wider.
A program may use at most 768 MiB of HBM per device.

```python
import jax
import jax.numpy as jnp
from jax import lax

D = 2048
HEADS = 16
HEAD = 128
EXPERTS = 64
TOP = 6
FE = 1408
FS = 2816
SEQ = 512
SEQS = 1
G = 8
CAP = 96

T = SEQS * SEQ
EPS = 1e-6


def _dot(a, b):
    return jnp.dot(a, b, preferred_element_type=jnp.float32)


def _rms(x, w):
    xf = x.astype(jnp.float32)
    r = lax.rsqrt(jnp.mean(xf * xf, axis=-1, keepdims=True) + EPS)
    return (xf * r * w.astype(jnp.float32)).astype(jnp.bfloat16)


def _rope(x):
    half = HEAD // 2
    freq = 10000.0 ** (-jnp.arange(half, dtype=jnp.float32) / half)
    ang = jnp.arange(SEQ, dtype=jnp.float32)[:, None] * freq[None, :]
    c = jnp.cos(ang)[:, None, :]
    s = jnp.sin(ang)[:, None, :]
    x1, x2 = x[..., :half], x[..., half:]
    return jnp.concatenate([x1 * c - x2 * s, x2 * c + x1 * s], axis=-1)


def _normal(key, shape, scale):
    return (jax.random.normal(key, shape, jnp.float32) * scale).astype(jnp.bfloat16)


def _scale(key):
    return jax.random.uniform(key, (D,), jnp.float32, 0.8, 1.2).astype(jnp.bfloat16)


def _expert_weight(weight_key):
    levels = jnp.sum(jax.random.randint(weight_key, (9, EXPERTS), 0, 10, jnp.int32), axis=0)
    hot_bias = 12 * (jnp.arange(EXPERTS) < EXPERTS // G).astype(jnp.int32)
    quarter = jnp.maximum(levels + hot_bias - 16, 0)
    return jnp.left_shift(4 + quarter % 4, quarter // 4).astype(jnp.int32)


def _route(route_key, weight):
    draw_rows = jax.random.bits(route_key, (T, TOP), jnp.uint32)

    def step(counts, draw_row):
        open_weight = jnp.where(counts < CAP, weight, 0).astype(jnp.int32)
        picked_list = []
        for choice in range(TOP):
            cumulative = jnp.cumsum(open_weight)
            total_weight = cumulative[-1].astype(jnp.uint32)
            target_val = (draw_row[choice] % total_weight).astype(jnp.int32)
            pick_id = jnp.searchsorted(cumulative, target_val, side='right').astype(jnp.int32)
            picked_list.append(pick_id)
            open_weight = open_weight.at[pick_id].set(0)
        chosen = jnp.stack(picked_list)
        return counts.at[chosen].add(1), (chosen, counts[chosen])

    _, (chosen, slots) = lax.scan(step, jnp.zeros((EXPERTS,), jnp.int32), draw_rows)
    return chosen.astype(jnp.int32), slots.astype(jnp.int32)


def setup_inputs(seed: int = 0, part: int = 0) -> dict:
    key = jax.random.PRNGKey(seed)
    kh, kr = jax.random.split(jax.random.fold_in(key, part))
    ks = jax.random.split(key, 15)
    hd = HEADS * HEAD
    expert_weight = _expert_weight(jax.random.fold_in(ks[14], 7))
    idx, slot = jax.vmap(lambda k: _route(k, expert_weight))(jax.random.split(kr, G))
    return {
        'h0': _normal(kh, (G * SEQS, SEQ, D), 1.0),
        'idx': idx.reshape(G * SEQS, SEQ, TOP),
        'slot': slot.reshape(G * SEQS, SEQ, TOP),
        'ln_attn': _scale(ks[0]),
        'wq': _normal(ks[1], (D, hd), 1.5 * D ** -0.5),
        'wk': _normal(ks[2], (D, hd), 1.5 * D ** -0.5),
        'wv': _normal(ks[3], (D, hd), D ** -0.5),
        'wo': _normal(ks[4], (hd, D), hd ** -0.5),
        'ln_ffn': _scale(ks[5]),
        'ws1': _normal(ks[6], (D, FS), D ** -0.5),
        'ws3': _normal(ks[7], (D, FS), D ** -0.5),
        'ws2': _normal(ks[8], (FS, D), FS ** -0.5),
        'ln_moe': _scale(ks[9]),
        'wr': _normal(ks[10], (D, EXPERTS), 1.5 * D ** -0.5),
        'ue1': _normal(ks[11], (EXPERTS, D, FE), D ** -0.5),
        'ue3': _normal(ks[12], (EXPERTS, D, FE), D ** -0.5),
        'ue2': _normal(ks[13], (EXPERTS, FE, D), 2.0 * FE ** -0.5),
    }


def reference(h0, idx, slot, ln_attn, wq, wk, wv, wo, ln_ffn, ws1, ws3, ws2, ln_moe, wr, ue1, ue3, ue2):
    nb = h0.shape[0]
    n = nb * SEQ
    x1 = _rms(h0, ln_attn)
    causal = jnp.arange(SEQ)[:, None] >= jnp.arange(SEQ)[None, :]

    def attn(xs):
        q = _rope(_dot(xs, wq).reshape(SEQ, HEADS, HEAD)).astype(jnp.bfloat16)
        k = _rope(_dot(xs, wk).reshape(SEQ, HEADS, HEAD)).astype(jnp.bfloat16)
        v = _dot(xs, wv).astype(jnp.bfloat16).reshape(SEQ, HEADS, HEAD)
        s = jnp.einsum('qhe,khe->hqk', q.astype(jnp.float32), k.astype(jnp.float32)) * HEAD ** -0.5
        p = jax.nn.softmax(jnp.where(causal[None], s, -1e30), axis=-1).astype(jnp.bfloat16)
        o = jnp.einsum('hqk,khe->qhe', p.astype(jnp.float32), v.astype(jnp.float32))
        return o.astype(jnp.bfloat16).reshape(SEQ, HEADS * HEAD)

    o = lax.map(attn, x1).reshape(n, HEADS * HEAD)
    h = h0.reshape(n, D)
    a = (h.astype(jnp.float32) + _dot(o, wo)).astype(jnp.bfloat16)
    x2 = _rms(a, ln_ffn)
    hs = (jax.nn.silu(_dot(x2, ws1)) * _dot(x2, ws3)).astype(jnp.bfloat16)
    f = _dot(hs, ws2)

    u = _rms(h, ln_moe)
    gi = idx.reshape(n, TOP)
    sl = slot.reshape(n, TOP)
    g = jax.nn.softmax(jnp.take_along_axis(_dot(u, wr), gi, axis=1), axis=-1)
    dev = jnp.arange(n, dtype=jnp.int32) // T
    pos = gi * (G * CAP) + dev[:, None] * CAP + sl
    src = jnp.full((EXPERTS * G * CAP,), n, jnp.int32).at[pos.reshape(-1)].set(
        jnp.arange(n * TOP, dtype=jnp.int32) // TOP)
    u_pad = jnp.concatenate([u, jnp.zeros((1, D), jnp.bfloat16)], axis=0)
    buf = u_pad[src].reshape(EXPERTS, G * CAP, D)

    def expert(args):
        x, w1, w3, w2 = args
        he = (jax.nn.silu(_dot(x, w1)) * _dot(x, w3)).astype(jnp.bfloat16)
        return _dot(he, w2).astype(jnp.bfloat16)

    y = lax.map(expert, (buf, ue1, ue3, ue2)).reshape(EXPERTS * G * CAP, D)
    m = jnp.sum(g[:, :, None] * y[pos].astype(jnp.float32), axis=1)
    out = a.astype(jnp.float32) + f + m
    return out.astype(jnp.bfloat16).reshape(nb, SEQ, D)
```

```python
import jax
import jax.numpy as jnp
from jax import lax
from jax.experimental import pallas as pl
from jax.experimental.pallas import tpu as pltpu
from jax.sharding import PartitionSpec as P

HEAD = 128
EPS = 1e-6
CAP_FACTOR = 2


def _mm(form, a, b):
    return jnp.einsum(form, a, b, preferred_element_type=jnp.float32)


def _rms(x, w):
    xf = x.astype(jnp.float32)
    r = lax.rsqrt(jnp.mean(xf * xf, axis=-1, keepdims=True) + EPS)
    return (xf * r * w.astype(jnp.float32)).astype(jnp.bfloat16)


def _rope(x):
    s, half = x.shape[1], x.shape[-1] // 2
    freq = 10000.0 ** (-jnp.arange(half, dtype=jnp.float32) / half)
    ang = jnp.arange(s, dtype=jnp.float32)[:, None] * freq[None, :]
    c = jnp.cos(ang)[None, :, None, :]
    sn = jnp.sin(ang)[None, :, None, :]
    x1, x2 = x[..., :half], x[..., half:]
    return jnp.concatenate([x1 * c - x2 * sn, x2 * c + x1 * sn], axis=-1)


def _dense(h0, ln_attn, wq, wk, wv, wo, ln_ffn, ws1, ws3, ws2):
    b, s, _ = h0.shape
    nh = wq.shape[1] // HEAD
    x1 = _rms(h0, ln_attn)
    q = _rope(_mm('bsd,de->bse', x1, wq).reshape(b, s, nh, HEAD)).astype(jnp.bfloat16)
    k = _rope(_mm('bsd,de->bse', x1, wk).reshape(b, s, nh, HEAD)).astype(jnp.bfloat16)
    v = _mm('bsd,de->bse', x1, wv).astype(jnp.bfloat16).reshape(b, s, nh, HEAD)
    sc = _mm('bqhe,bkhe->bhqk', q, k) * HEAD ** -0.5
    causal = jnp.arange(s)[:, None] >= jnp.arange(s)[None, :]
    p = jax.nn.softmax(jnp.where(causal, sc, -1e30), axis=-1).astype(jnp.bfloat16)
    o = _mm('bhqk,bkhe->bqhe', p, v).astype(jnp.bfloat16).reshape(b, s, nh * HEAD)
    a = (h0.astype(jnp.float32) + _mm('bse,ed->bsd', o, wo)).astype(jnp.bfloat16)
    x2 = _rms(a, ln_ffn)
    hs = (jax.nn.silu(_mm('bsd,df->bsf', x2, ws1)) * _mm('bsd,df->bsf', x2, ws3)).astype(jnp.bfloat16)
    return a, _mm('bsf,fd->bsd', hs, ws2)


VMEM_LIMIT = 66_000_000
LANES = 128
COLS = 256
MESH = pl.DeviceIdType.MESH


def _dispatch_kernel(el, cap, top, base_ref, ug_ref, wr_ref, x_ref, hit_ref, gr_ref):
    t = hit_ref.shape[-1]
    ne = wr_ref.shape[-1]
    meta = ug_ref[0, t:t + 16, :t].astype(jnp.float32)
    idx = meta[0:top].astype(jnp.int32)
    row = idx * cap + meta[8:8 + top].astype(jnp.int32) - base_ref[0]
    lg = lax.dot_general(wr_ref[...], ug_ref[0, :t, :], (((0,), (1,)), ((), ())), preferred_element_type=jnp.float32)
    expert = lax.broadcasted_iota(jnp.int32, (ne, t), 0)
    picked = [jnp.sum(jnp.where(expert == idx[j:j + 1], lg, 0.0), axis=0, keepdims=True) for j in range(top)]
    high = picked[0]
    for p in picked[1:]:
        high = jnp.maximum(high, p)
    ex = [jnp.exp(p - high) for p in picked]
    den = ex[0]
    for e in ex[1:]:
        den = den + e
    gate = [e / den for e in ex]
    for e in range(el):
        at = lax.broadcasted_iota(jnp.int32, (cap, t), 0) + e * cap
        hit = jnp.zeros((cap, t), jnp.float32)
        g = jnp.zeros((cap, t), jnp.float32)
        for j in range(top):
            same = at == row[j:j + 1]
            hit = jnp.where(same, 1.0, hit)
            g = jnp.where(same, gate[j], g)
        hit_ref[0, e * cap:(e + 1) * cap, :] = hit.astype(jnp.bfloat16)
        gr_ref[0, e * cap:(e + 1) * cap, :] = jnp.broadcast_to(jnp.sum(g, axis=1, keepdims=True), (cap, LANES))
    half = el // 2

    def column(c, _):
        cols = pl.ds(pl.multiple_of(c * COLS, COLS), COLS)
        x = jnp.dot(hit_ref[0], ug_ref[0, :t, cols], preferred_element_type=jnp.float32)
        x_ref[:, 0, :, cols] = x.astype(jnp.bfloat16).reshape(el, cap, COLS)
        return 0

    lax.fori_loop(0, x_ref.shape[-1] // COLS, column, 0)


def _dispatch(base, ug, wr, el, cap, top):
    g, rows, d = ug.shape
    t = rows - 16
    n = el * cap
    return pl.pallas_call(
        lambda *refs: _dispatch_kernel(el, cap, top, *refs),
        grid=(g,),
        in_specs=[
            pl.BlockSpec(memory_space=pltpu.SMEM),
            pl.BlockSpec((1, rows, d), lambda i: (i, 0, 0)),
            pl.BlockSpec(wr.shape, lambda i: (0, 0)),
        ],
        out_specs=[
            pl.BlockSpec((el, 1, cap, d), lambda i: (0, i, 0, 0)),
            pl.BlockSpec((1, n, t), lambda i: (i, 0, 0)),
            pl.BlockSpec((1, n, LANES), lambda i: (i, 0, 0)),
        ],
        out_shape=[
            jax.ShapeDtypeStruct((el, g, cap, d), jnp.bfloat16),
            jax.ShapeDtypeStruct((g, n, t), jnp.bfloat16),
            jax.ShapeDtypeStruct((g, n, LANES), jnp.float32),
        ],
        compiler_params=pltpu.CompilerParams(vmem_limit_bytes=VMEM_LIMIT),
        cost_estimate=pl.CostEstimate(flops=2 * g * n * t * d, bytes_accessed=60_000_000, transcendentals=0),
        name='dispatch',
    )(base, ug, wr)


def _up_kernel(x_ref, w1_ref, w3_ref, h_ref):
    def column(c, _):
        cols = pl.ds(pl.multiple_of(c * LANES, LANES), LANES)
        w = jnp.concatenate([w1_ref[0, :, cols], w3_ref[0, :, cols]], axis=1)
        r = jnp.dot(x_ref[0], w, preferred_element_type=jnp.float32)
        h_ref[0, :, cols] = (jax.nn.silu(r[:, :LANES]) * r[:, LANES:]).astype(jnp.bfloat16)
        return 0

    lax.fori_loop(0, h_ref.shape[-1] // LANES, column, 0)


def _up(x, ue1, ue3):
    el, n, d = x.shape
    f = ue1.shape[-1]
    return pl.pallas_call(
        _up_kernel,
        grid=(el,),
        in_specs=[
            pl.BlockSpec((1, n, d), lambda i: (i, 0, 0)),
            pl.BlockSpec((1, d, f), lambda i: (i, 0, 0)),
            pl.BlockSpec((1, d, f), lambda i: (i, 0, 0)),
        ],
        out_specs=pl.BlockSpec((1, n, f), lambda i: (i, 0, 0)),
        out_shape=jax.ShapeDtypeStruct((el, n, f), jnp.bfloat16),
        compiler_params=pltpu.CompilerParams(vmem_limit_bytes=VMEM_LIMIT),
        cost_estimate=pl.CostEstimate(flops=4 * el * n * f * d, bytes_accessed=100_000_000, transcendentals=0),
        name='up',
    )(x, ue1, ue3)


def _down_kernel(nc, g, he_hbm, w_hbm, hit_hbm, gr_hbm, out_ref,
                 he, w, hit, gr, y, p, ra, rb, rf,
                 he_sem, w_sem, in_sem, a_send, a_recv, b_send, b_recv, f_send, f_recv, a_free, b_free, f_free):
    el, n, f = he.shape
    t = hit.shape[-1]
    cap = n // g
    chips = g // 2
    me = lax.axis_index('ep')
    core, chip = lax.rem(me, 2), lax.div(me, 2)
    lchip, rchip, ochip = lax.rem(chip + chips - 1, chips), lax.rem(chip + 1, chips), lax.rem(chip + 2, chips)
    mate, left, right = me + 1 - 2 * core, 2 * lchip + core, 2 * rchip + core

    def he_copy(e):
        return pltpu.make_async_copy(he_hbm.at[e], he.at[e], he_sem.at[e])

    def w_copy(q):
        e, c, slot = lax.rem(q, el), lax.div(q, el), lax.rem(q, 4)
        cols = pl.ds(pl.multiple_of(c * COLS, COLS), COLS)
        return pltpu.make_async_copy(w_hbm.at[e, :, cols], w.at[slot], w_sem.at[slot])

    hit_copy = pltpu.make_async_copy(hit_hbm, hit, in_sem.at[0])
    gr_copy = pltpu.make_async_copy(gr_hbm, gr, in_sem.at[1])

    def a_copy(c):
        return pltpu.make_async_remote_copy(
            src_ref=p.at[lax.rem(c, 3), 1 - core], dst_ref=ra.at[lax.rem(c, 2)],
            send_sem=a_send.at[lax.rem(c, 2)], recv_sem=a_recv.at[lax.rem(c, 2)],
            device_id={'ep': mate}, device_id_type=MESH)

    def b_copy(c, way):
        return pltpu.make_async_remote_copy(
            src_ref=p.at[lax.rem(c, 3), core, ochip, :, pl.ds(way * LANES, LANES)], dst_ref=rb.at[lax.rem(c, 2), way],
            send_sem=b_send.at[lax.rem(c, 3), way], recv_sem=b_recv.at[lax.rem(c, 2), way],
            device_id={'ep': (left, right)[way]}, device_id_type=MESH)

    def f_copy(c, way):
        return pltpu.make_async_remote_copy(
            src_ref=p.at[lax.rem(c, 3), core, (lchip, rchip)[way]], dst_ref=rf.at[lax.rem(c, 2), way],
            send_sem=f_send.at[lax.rem(c, 3), way], recv_sem=f_recv.at[lax.rem(c, 2), way],
            device_id={'ep': (left, right)[way]}, device_id_type=MESH)

    def signal(sem, dev):
        pl.semaphore_signal(sem, inc=1, device_id={'ep': dev}, device_id_type=MESH)

    w_copy(0).start()
    for e in range(el):
        he_copy(e).start()
        if e < 2:
            w_copy(e + 1).start()
    hit_copy.start()
    gr_copy.start()

    barrier = pltpu.get_barrier_semaphore()
    for dev in (mate, left, right):
        signal(barrier, dev)
    pl.semaphore_wait(barrier, 3)

    def chunk(i, _):
        @pl.when(i < nc)
        def _():
            def expert(e, _):
                q = i * el + e

                @pl.when(q + 3 < nc * el)
                def _():
                    w_copy(q + 3).start()

                @pl.when(i == 0)
                def _():
                    he_copy(e).wait()

                w_copy(q).wait()
                yy = jnp.dot(he[e], w[lax.rem(q, 4)], preferred_element_type=jnp.float32)
                y[:, e] = yy.astype(jnp.bfloat16).reshape(g, cap, COLS)
                return 0

            lax.fori_loop(0, el, expert, 0)

        @pl.when(jnp.logical_and(i >= 1, i <= nc))
        def _():
            c = i - 1
            slot = lax.rem(c, 3)
            cc = a_copy(c)
            cc.wait_recv()
            cc.wait_send()
            p[slot, core] += ra[lax.rem(c, 2)]

            @pl.when(c < nc - 2)
            def _():
                signal(a_free, mate)

            @pl.when(c >= 2)
            def _():
                pl.semaphore_wait(b_free.at[0], 1)
                pl.semaphore_wait(b_free.at[1], 1)

            b_copy(c, 0).start()
            b_copy(c, 1).start()

        @pl.when(jnp.logical_and(i >= 2, i <= nc + 1))
        def _():
            c = i - 2
            slot = lax.rem(c, 3)
            b_copy(c, 0).wait_recv()
            b_copy(c, 1).wait_recv()
            p[slot, core, lchip, :, :LANES] += rb[lax.rem(c, 2), 0]
            p[slot, core, rchip, :, LANES:] += rb[lax.rem(c, 2), 1]

            @pl.when(c < nc - 2)
            def _():
                signal(b_free.at[0], right)
                signal(b_free.at[1], left)

            @pl.when(c >= 2)
            def _():
                pl.semaphore_wait(f_free.at[0], 1)
                pl.semaphore_wait(f_free.at[1], 1)

            f_copy(c, 0).start()
            f_copy(c, 1).start()

        @pl.when(i >= 3)
        def _():
            c = i - 3
            f_copy(c, 0).wait_recv()
            f_copy(c, 1).wait_recv()
            cols = pl.ds(pl.multiple_of(c * COLS, COLS), COLS)
            out_ref[:, cols] = p[lax.rem(c, 3), core, chip] + (rf[lax.rem(c, 2), 0] + rf[lax.rem(c, 2), 1])

            @pl.when(c < nc - 2)
            def _():
                signal(f_free.at[0], right)
                signal(f_free.at[1], left)

            for way in range(2):
                b_copy(c, way).wait_send()
                f_copy(c, way).wait_send()

        @pl.when(i < nc)
        def _():
            @pl.when(i == 0)
            def _():
                hit_copy.wait()
                gr_copy.wait()

            slot = lax.rem(i, 3)

            def combine(kk):
                def dest(dc, _):
                    dd = 2 * dc + kk
                    scale = gr[dd]
                    z = y[dd].reshape(n, COLS).astype(jnp.float32) * jnp.concatenate([scale, scale], axis=1)
                    hi = z.astype(jnp.bfloat16)
                    z = z - hi.astype(jnp.float32)
                    mid = z.astype(jnp.bfloat16)
                    lo = (z - mid.astype(jnp.float32)).astype(jnp.bfloat16)
                    r = lax.dot_general(hit[dd], jnp.concatenate([hi, mid, lo], axis=1), (((0,), (0,)), ((), ())),
                                        preferred_element_type=jnp.float32)
                    p[slot, kk, dc] = r[:, :COLS] + (r[:, COLS:2 * COLS] + r[:, 2 * COLS:])
                    return 0

                lax.fori_loop(0, chips, dest, 0)

            combine(1 - core)

            @pl.when(i >= 2)
            def _():
                pl.semaphore_wait(a_free, 1)

            a_copy(i).start()
            combine(core)

        return 0

    lax.fori_loop(0, nc + 3, chunk, 0)


def _down(he, ue2, hit, gr, g):
    el, n, f = he.shape
    d = ue2.shape[-1]
    t = hit.shape[-1]
    nc = d // COLS
    chips = g // 2
    dma = pltpu.SemaphoreType.DMA
    reg = pltpu.SemaphoreType.REGULAR
    return pl.pallas_call(
        lambda *refs: _down_kernel(nc, g, *refs),
        in_specs=[pl.BlockSpec(memory_space=pl.ANY)] * 4,
        out_specs=pl.BlockSpec(memory_space=pltpu.VMEM),
        out_shape=jax.ShapeDtypeStruct((t, d), jnp.float32),
        scratch_shapes=[
            pltpu.VMEM((el, n, f), jnp.bfloat16),
            pltpu.VMEM((4, f, COLS), jnp.bfloat16),
            pltpu.VMEM(hit.shape, jnp.bfloat16),
            pltpu.VMEM(gr.shape, jnp.float32),
            pltpu.VMEM((g, el, n // g, COLS), jnp.bfloat16),
            pltpu.VMEM((3, 2, chips, t, COLS), jnp.float32),
            pltpu.VMEM((2, chips, t, COLS), jnp.float32),
            pltpu.VMEM((2, 2, t, LANES), jnp.float32),
            pltpu.VMEM((2, 2, t, COLS), jnp.float32),
            dma((el,)), dma((4,)), dma((2,)),
            dma((2,)), dma((2,)), dma((3, 2)), dma((2, 2)), dma((3, 2)), dma((2, 2)),
            reg, reg((2,)), reg((2,)),
        ],
        compiler_params=pltpu.CompilerParams(vmem_limit_bytes=VMEM_LIMIT, collective_id=0, has_side_effects=True),
        cost_estimate=pl.CostEstimate(flops=2 * el * n * f * d + 6 * g * n * t * d, bytes_accessed=60_000_000, transcendentals=0),
        name='down',
    )(he, ue2, hit, gr)


def solution(mesh):
    g_ = mesh.shape['ep']
    rows = P(('dp', 'ep'))
    rep = P()

    def local(h0, idx, slot, ln_attn, wq, wk, wv, wo, ln_ffn, ws1, ws3, ws2, ln_moe, wr, ue1, ue3, ue2):
        b, s, d = h0.shape
        top = idx.shape[-1]
        el = ue1.shape[0]
        ne = el * g_
        t = b * s
        cap = CAP_FACTOR * t * top // ne
        u = _rms(h0, ln_moe).reshape(t, d)
        meta = jnp.zeros((16, d), jnp.bfloat16)
        meta = meta.at[0:top, :t].set(idx.reshape(t, top).T.astype(jnp.bfloat16))
        meta = meta.at[8:8 + top, :t].set(slot.reshape(t, top).T.astype(jnp.bfloat16))
        ug = lax.all_gather(jnp.concatenate([u, meta], axis=0), 'ep')
        a, fo = _dense(h0, ln_attn, wq, wk, wv, wo, ln_ffn, ws1, ws3, ws2)
        base = (lax.axis_index('ep') * (el * cap)).astype(jnp.int32).reshape(1)
        x, hit, gr = _dispatch(base, ug, wr, el, cap, top)
        he = _up(x.reshape(el, g_ * cap, d), ue1, ue3)
        m = _down(he, ue2, hit, gr, g_)
        out = a.astype(jnp.float32) + fo + m.reshape(b, s, d)
        return out.astype(jnp.bfloat16)

    specs = (rows, rows, rows) + (rep,) * 11 + (P('ep'), P('ep'), P('ep'))
    return jax.shard_map(local, mesh=mesh, in_specs=specs, out_specs=rows, check_vma=False)
```

```python
import jax
import jax.numpy as jnp
from jax import lax
from jax.experimental import pallas as pl
from jax.experimental.pallas import tpu as pltpu
from jax.sharding import PartitionSpec as P

HEAD = 128
EPS = 1e-6
CAP_FACTOR = 2


def _rms(x, w):
    xf = x.astype(jnp.float32)
    r = lax.rsqrt(jnp.mean(xf * xf, axis=-1, keepdims=True) + EPS)
    return (xf * r * w.astype(jnp.float32)).astype(jnp.bfloat16)


def _dot(a, b):
    return jnp.dot(a, b, preferred_element_type=jnp.float32)


def _angles(s):
    half = HEAD // 2
    freq = 10000.0 ** (-jnp.arange(half, dtype=jnp.float32) / half)
    ang = jnp.arange(s, dtype=jnp.float32)[:, None] * freq[None, :]
    c, sn = jnp.cos(ang), jnp.sin(ang)
    return jnp.concatenate([c, c], axis=1), jnp.concatenate([-sn, sn], axis=1)


def _attention_kernel(h_ref, ln_ref, cos_ref, sin_ref, wq_ref, wk_ref, wv_ref, o_ref, x_ref):
    s = h_ref.shape[0]
    block = s // 2

    @pl.when(pl.program_id(0) == 0)
    def _():
        x_ref[...] = _rms(h_ref[...], ln_ref[...])

    def rope(z):
        return (z * cos_ref[...] + pltpu.roll(z, HEAD // 2, 1) * sin_ref[...]).astype(jnp.bfloat16)

    q2, k2 = _dot(x_ref[...], wq_ref[...]), _dot(x_ref[...], wk_ref[...])
    v2 = _dot(x_ref[...], wv_ref[...]).astype(jnp.bfloat16)
    for h in range(q2.shape[1] // HEAD):
        cols = slice(h * HEAD, (h + 1) * HEAD)
        q, k, v = rope(q2[:, cols]), rope(k2[:, cols]), v2[:, cols]
        for b in range(2):
            n = (b + 1) * block
            sc = lax.dot_general(q[b * block:n], k[:n], (((1,), (1,)), ((), ())), preferred_element_type=jnp.float32)
            at = lax.broadcasted_iota(jnp.int32, (block, n), 0) + b * block
            sc = jnp.where(at >= lax.broadcasted_iota(jnp.int32, (block, n), 1), sc * HEAD ** -0.5, -1e30)
            e = jnp.exp(sc - jnp.max(sc, axis=1, keepdims=True))
            p = (e * (1.0 / jnp.sum(e, axis=1, keepdims=True))).astype(jnp.bfloat16)
            o_ref[b * block:n, cols] = _dot(p, v[:n]).astype(jnp.bfloat16)


def _attention(h, ln, wq, wk, wv):
    s, d = h.shape
    e = wq.shape[1]
    cos, sin = _angles(s)
    whole = lambda i: (0, 0)
    strip = pl.BlockSpec((d, 2 * HEAD), lambda i: (0, i))
    return pl.pallas_call(
        _attention_kernel,
        grid=(e // (2 * HEAD),),
        in_specs=[pl.BlockSpec((s, d), whole), pl.BlockSpec((1, d), whole), pl.BlockSpec((s, HEAD), whole),
                  pl.BlockSpec((s, HEAD), whole), strip, strip, strip],
        out_specs=pl.BlockSpec((s, 2 * HEAD), lambda i: (0, i)),
        out_shape=jax.ShapeDtypeStruct((s, e), jnp.bfloat16),
        scratch_shapes=[pltpu.VMEM((s, d), jnp.bfloat16)],
        compiler_params=pltpu.CompilerParams(vmem_limit_bytes=VMEM_LIMIT),
        cost_estimate=pl.CostEstimate(flops=6 * s * d * e + 4 * s * s * e, bytes_accessed=6 * d * e, transcendentals=0),
        name='attention',
    )(h, ln.reshape(1, d), cos, sin, wq, wk, wv)


def _ffn_kernel(n1, n2, h_ref, o_ref, ln_ref, wo_ref, w1_ref, w3_ref, w2_ref, out_ref, a_ref, x_ref, s_ref):
    i = pl.program_id(0)

    @pl.when(i < n1)
    def _():
        w = wo_ref.shape[1]
        cols = pl.ds(pl.multiple_of(i * w, w), w)
        a_ref[:, cols] = (h_ref[:, cols].astype(jnp.float32) + _dot(o_ref[...], wo_ref[...])).astype(jnp.bfloat16)

    @pl.when(i == n1)
    def _():
        x_ref[...] = _rms(a_ref[...], ln_ref[...])

    @pl.when(jnp.logical_and(i >= n1, i < n1 + n2))
    def _():
        w = w1_ref.shape[1]
        cols = pl.ds(pl.multiple_of((i - n1) * w, w), w)
        s_ref[:, cols] = (jax.nn.silu(_dot(x_ref[...], w1_ref[...])) * _dot(x_ref[...], w3_ref[...])).astype(jnp.bfloat16)

    @pl.when(i >= n1 + n2)
    def _():
        w = w2_ref.shape[1]
        cols = pl.ds(pl.multiple_of((i - n1 - n2) * w, w), w)
        out_ref[...] = a_ref[:, cols].astype(jnp.float32) + _dot(s_ref[...], w2_ref[...])


def _ffn(h, o, ln, wo, ws1, ws3, ws2):
    s, d = h.shape
    e, f = wo.shape[0], ws1.shape[1]
    c1, c2 = 512, 256
    n1, n2 = d // c1, f // c2
    whole = lambda i: (0, 0)
    clip = lambda x, hi: jnp.minimum(jnp.maximum(x, 0), hi)
    mid = pl.BlockSpec((d, c2), lambda i: (0, clip(i - n1, n2 - 1)))
    return pl.pallas_call(
        lambda *refs: _ffn_kernel(n1, n2, *refs),
        grid=(2 * n1 + n2,),
        in_specs=[pl.BlockSpec((s, d), whole), pl.BlockSpec((s, e), whole), pl.BlockSpec((1, d), whole),
                  pl.BlockSpec((e, c1), lambda i: (0, clip(i, n1 - 1))), mid, mid,
                  pl.BlockSpec((f, c1), lambda i: (0, clip(i - n1 - n2, n1 - 1)))],
        out_specs=pl.BlockSpec((s, c1), lambda i: (0, clip(i - n1 - n2, n1 - 1))),
        out_shape=jax.ShapeDtypeStruct((s, d), jnp.float32),
        scratch_shapes=[pltpu.VMEM((s, d), jnp.bfloat16), pltpu.VMEM((s, d), jnp.bfloat16), pltpu.VMEM((s, f), jnp.bfloat16)],
        compiler_params=pltpu.CompilerParams(vmem_limit_bytes=VMEM_LIMIT),
        cost_estimate=pl.CostEstimate(flops=2 * s * d * e + 6 * s * d * f, bytes_accessed=2 * d * e + 6 * d * f, transcendentals=0),
        name='ffn',
    )(h, o, ln.reshape(1, d), wo, ws1, ws3, ws2)


VMEM_LIMIT = 66_000_000
LANES = 128
COLS = 256
UE = 8
UD = 4
MESH = pl.DeviceIdType.MESH


def _dispatch_kernel(el, cap, top, base_ref, order_ref, ug_ref, wr_ref, x_ref, back_ref, gr_ref, hit_ref):
    t = hit_ref.shape[-1]
    ne = wr_ref.shape[-1]
    meta = ug_ref[0, t:t + 16, :t].astype(jnp.float32)
    idx = meta[0:top].astype(jnp.int32)
    row = idx * cap + meta[8:8 + top].astype(jnp.int32) - base_ref[0]
    lg = _dot(ug_ref[0, :t, :], wr_ref[...]).T
    expert = lax.broadcasted_iota(jnp.int32, (ne, t), 0)
    picked = [jnp.sum(jnp.where(expert == idx[j:j + 1], lg, 0.0), axis=0, keepdims=True) for j in range(top)]
    high = picked[0]
    for p in picked[1:]:
        high = jnp.maximum(high, p)
    ex = [jnp.exp(p - high) for p in picked]
    den = ex[0]
    for e in ex[1:]:
        den = den + e
    gate = [e / den for e in ex]
    col = jnp.concatenate([row, jnp.zeros((16 - top, t), jnp.int32)], axis=0).astype(jnp.float32).T.astype(jnp.int32)
    n = el * cap
    step, wide, blocks = 32, 2 * COLS, 2

    def build(r):
        at = lax.broadcasted_iota(jnp.int32, (step, t), 0) + r
        hit = jnp.zeros((step, t), jnp.float32)
        g = jnp.zeros((step, t), jnp.float32)
        for j in range(top):
            same = at == row[j:j + 1]
            hit = jnp.where(same, 1.0, hit)
            g = jnp.where(same, gate[j], g)
        hit_ref[r:r + step, :] = hit.astype(jnp.bfloat16)
        gr_ref[0, r:r + step, :] = jnp.broadcast_to(jnp.sum(g, axis=1, keepdims=True), (step, LANES))

    def build_back(r):
        at = lax.broadcasted_iota(jnp.int32, (step, n), 1)
        back = jnp.zeros((step, n), jnp.float32)
        for j in range(top):
            back = jnp.where(at == col[r:r + step, j:j + 1], 1.0, back)
        back_ref[0, r:r + step, :] = back.astype(jnp.bfloat16)

    part = n // blocks
    for h in range(blocks):
        for r in range(h * part, (h + 1) * part, step):
            build(r)
        for c in range(x_ref.shape[-1] // wide):
            cols = slice(c * wide, (c + 1) * wide)
            x = _dot(hit_ref[h * part:(h + 1) * part], ug_ref[0, :t, cols])
            x_ref[h * part // cap:(h + 1) * part // cap, 0, :, cols] = x.astype(jnp.bfloat16).reshape(part // cap, cap, wide)
    for r in range(0, t, step):
        build_back(r)


def _dispatch(base, order, ug, wr, el, cap, top):
    g = order.shape[0]
    _, rows, d = ug.shape
    t = rows - 16
    n = el * cap
    return pl.pallas_call(
        lambda *refs: _dispatch_kernel(el, cap, top, *refs),
        grid_spec=pltpu.PrefetchScalarGridSpec(
            num_scalar_prefetch=2,
            grid=(g,),
            in_specs=[
                pl.BlockSpec((1, rows, d), lambda i, base, order: (order[i], 0, 0)),
                pl.BlockSpec(wr.shape, lambda i, base, order: (0, 0)),
            ],
            out_specs=[
                pl.BlockSpec((el, 1, cap, d), lambda i, base, order: (0, i, 0, 0)),
                pl.BlockSpec((1, t, n), lambda i, base, order: (i, 0, 0)),
                pl.BlockSpec((1, n, LANES), lambda i, base, order: (i, 0, 0)),
            ],
            scratch_shapes=[pltpu.VMEM((n, t), jnp.bfloat16)],
        ),
        out_shape=[
            jax.ShapeDtypeStruct((el, g, cap, d), jnp.bfloat16),
            jax.ShapeDtypeStruct((g, t, n), jnp.bfloat16),
            jax.ShapeDtypeStruct((g, n, LANES), jnp.float32),
        ],
        compiler_params=pltpu.CompilerParams(vmem_limit_bytes=VMEM_LIMIT),
        cost_estimate=pl.CostEstimate(flops=2 * g * n * t * d, bytes_accessed=8_000_000 * g, transcendentals=0),
        name='dispatch',
    )(base, order, ug, wr)


def _up_kernel(x_ref, w1_ref, w3_ref, h_ref):
    for c in range(h_ref.shape[-1] // LANES):
        cols = slice(c * LANES, (c + 1) * LANES)
        r = _dot(x_ref[0], jnp.concatenate([w1_ref[0, :, cols], w3_ref[0, :, cols]], axis=1))
        h_ref[0, :, cols] = (jax.nn.silu(r[:, :LANES]) * r[:, LANES:]).astype(jnp.bfloat16)


def _up(x, ue1, ue3):
    el, n, d = x.shape
    f = ue1.shape[-1]
    return pl.pallas_call(
        _up_kernel,
        grid=(el,),
        in_specs=[
            pl.BlockSpec((1, n, d), lambda i: (i, 0, 0)),
            pl.BlockSpec((1, d, f), lambda i: (i, 0, 0)),
            pl.BlockSpec((1, d, f), lambda i: (i, 0, 0)),
        ],
        out_specs=pl.BlockSpec((1, n, f), lambda i: (i, 0, 0)),
        out_shape=jax.ShapeDtypeStruct((el, n, f), jnp.bfloat16),
        compiler_params=pltpu.CompilerParams(vmem_limit_bytes=VMEM_LIMIT),
        cost_estimate=pl.CostEstimate(flops=4 * el * n * f * d, bytes_accessed=100_000_000, transcendentals=0),
        name='up',
    )(x, ue1, ue3)


def _down_kernel(nc, g, he_hbm, w_hbm, hit_hbm, gr_hbm, out_ref,
                 he, w, hit, gr, y, p, ra, rb, rf,
                 he_sem, w_sem, in_sem, a_send, a_recv, b_send, b_recv, f_send, f_recv, a_free, b_free, f_free, out_sem):
    el, n, f = he.shape
    t = hit.shape[1]
    cap = n // g
    chips = g // 2
    me = lax.axis_index('ep')
    core, chip = lax.rem(me, 2), lax.div(me, 2)
    mate = me + 1 - 2 * core
    left, right = 2 * lax.rem(chip + chips - 1, chips) + core, 2 * lax.rem(chip + 1, chips) + core
    lchip, rchip, ochip, chip, core = chips - 1, 1, chips // 2, 0, 0

    def he_copy(e):
        return pltpu.make_async_copy(he_hbm.at[e], he.at[e], he_sem.at[e])

    def w_copy(q):
        e, c = lax.rem(q, el), lax.div(q, el)
        cols = pl.ds(pl.multiple_of(c * COLS, COLS), COLS)
        return pltpu.make_async_copy(w_hbm.at[e, :, cols], w.at[lax.rem(c, 2), e], w_sem.at[lax.rem(c, 2), e])

    in_copies = [pltpu.make_async_copy(hit_hbm, hit, in_sem.at[0]), pltpu.make_async_copy(gr_hbm, gr, in_sem.at[1])]

    def a_copy(c):
        return pltpu.make_async_remote_copy(
            src_ref=p.at[lax.rem(c, 3), 1], dst_ref=ra.at[lax.rem(c, 2)],
            send_sem=a_send.at[lax.rem(c, 2)], recv_sem=a_recv.at[lax.rem(c, 2)],
            device_id={'ep': mate}, device_id_type=MESH)

    def b_copy(c, way):
        return pltpu.make_async_remote_copy(
            src_ref=p.at[lax.rem(c, 3), 0, ochip, :, pl.ds(way * LANES, LANES)], dst_ref=rb.at[lax.rem(c, 2), way],
            send_sem=b_send.at[lax.rem(c, 2), way], recv_sem=b_recv.at[lax.rem(c, 2), way],
            device_id={'ep': (left, right)[way]}, device_id_type=MESH)

    def f_copy(c, way):
        return pltpu.make_async_remote_copy(
            src_ref=p.at[lax.rem(c, 3), 0, (lchip, rchip)[way]], dst_ref=rf.at[lax.rem(c, 2), way],
            send_sem=f_send.at[lax.rem(c, 2), way], recv_sem=f_recv.at[lax.rem(c, 2), way],
            device_id={'ep': (left, right)[way]}, device_id_type=MESH)

    def signal(sem, dev):
        pl.semaphore_signal(sem, inc=1, device_id={'ep': dev}, device_id_type=MESH)

    for e in range(el):
        w_copy(e).start()
        he_copy(e).start()
    for copy in in_copies:
        copy.start()

    barrier = pltpu.get_barrier_semaphore()
    for dev in (mate, left, right):
        signal(barrier, dev)
    pl.semaphore_wait(barrier, 3)

    def chunk(i, _):
        q0 = i * el

        @pl.when(i < nc)
        def _():
            @pl.when(i == 0)
            def _():
                for e in range(el):
                    he_copy(e).wait()
                for copy in in_copies:
                    copy.wait()

            @pl.when(i + 1 < nc)
            def _():
                for e in range(el):
                    w_copy(q0 + el + e).start()

            for e in range(el):
                w_copy(q0 + e).wait()

            def expert(e, _):
                q = q0 + e

                yy = jnp.dot(he[e], w[lax.rem(i, 2), e], preferred_element_type=jnp.float32)
                y[:, e] = yy.astype(jnp.bfloat16).reshape(g, cap, COLS)
                return 0

            lax.fori_loop(0, el, expert, 0, unroll=UE)


        @pl.when(jnp.logical_and(i >= 2, i <= nc + 1))
        def _():
            c = i - 2
            s, k = lax.rem(c, 3), lax.rem(c, 2)
            for way in range(2):
                b_copy(c, way).wait_recv()
                b_copy(c, way).wait_send()
            p[s, 0, lchip, :, :LANES] += rb[k, 0]
            p[s, 0, rchip, :, LANES:] += rb[k, 1]

            @pl.when(c < nc - 2)
            def _():
                signal(b_free.at[0], right)
                signal(b_free.at[1], left)

            @pl.when(c >= 2)
            def _():
                pl.semaphore_wait(f_free.at[0], 1)
                pl.semaphore_wait(f_free.at[1], 1)

            f_copy(c, 0).start()
            f_copy(c, 1).start()

        @pl.when(i >= 3)
        def _():
            c = i - 3
            s, k = lax.rem(c, 3), lax.rem(c, 2)
            f_copy(c, 0).wait_recv()
            f_copy(c, 1).wait_recv()
            rf[k, 0] = p[s, 0, 0] + (rf[k, 0] + rf[k, 1])
            f_copy(c, 0).wait_send()
            f_copy(c, 1).wait_send()
            cols = pl.ds(pl.multiple_of(c * COLS, COLS), COLS)
            done = pltpu.make_async_copy(rf.at[k, 0], out_ref.at[:, cols], out_sem)
            done.start()
            done.wait()

            @pl.when(c < nc - 2)
            def _():
                signal(f_free.at[0], right)
                signal(f_free.at[1], left)

        @pl.when(i < nc)
        def _():
            s = lax.rem(i, 3)

            def combine(side):
                def dest(dc, _):
                    dd = 2 * dc + side
                    scale = gr[dd]
                    z = y[dd].reshape(n, COLS).astype(jnp.float32) * jnp.concatenate([scale, scale], axis=1)
                    hi = z.astype(jnp.bfloat16)
                    z = z - hi.astype(jnp.float32)
                    mid = z.astype(jnp.bfloat16)
                    lo = (z - mid.astype(jnp.float32)).astype(jnp.bfloat16)
                    r = _dot(hit[dd], jnp.concatenate([hi, mid, lo], axis=1))
                    p[s, side, dc] = r[:, :COLS] + (r[:, COLS:2 * COLS] + r[:, 2 * COLS:])
                    return 0

                lax.fori_loop(0, chips, dest, 0, unroll=UD)

            combine(1)

            @pl.when(i >= 2)
            def _():
                pl.semaphore_wait(a_free, 1)

            a_copy(i).start()
            combine(0)
            cc = a_copy(i)
            cc.wait_recv()
            cc.wait_send()
            k = lax.rem(i, 2)
            p[s, 0, ochip] += ra[k, ochip]
            for r in (0, 1, chips - 1):
                p[s, 0, r] += ra[k, r]

            @pl.when(i < nc - 2)
            def _():
                signal(a_free, mate)

            @pl.when(i >= 2)
            def _():
                pl.semaphore_wait(b_free.at[0], 1)
                pl.semaphore_wait(b_free.at[1], 1)

            b_copy(i, 0).start()
            b_copy(i, 1).start()

        return 0

    lax.fori_loop(0, nc + 3, chunk, 0)


def _down(he, ue2, hit, gr):
    el, n, f = he.shape
    g, t, _ = hit.shape
    d = ue2.shape[-1]
    nc = d // COLS
    chips = g // 2
    dma = pltpu.SemaphoreType.DMA
    reg = pltpu.SemaphoreType.REGULAR
    return pl.pallas_call(
        lambda *refs: _down_kernel(nc, g, *refs),
        in_specs=[pl.BlockSpec(memory_space=pl.ANY)] * 4,
        out_specs=pl.BlockSpec(memory_space=pl.ANY),
        out_shape=jax.ShapeDtypeStruct((t, d), jnp.float32),
        scratch_shapes=[
            pltpu.VMEM((el, n, f), jnp.bfloat16),
            pltpu.VMEM((2, el, f, COLS), jnp.bfloat16),
            pltpu.VMEM((g, t, n), jnp.bfloat16),
            pltpu.VMEM((g, n, LANES), jnp.float32),
            pltpu.VMEM((g, el, n // g, COLS), jnp.bfloat16),
            pltpu.VMEM((3, 2, chips, t, COLS), jnp.float32),
            pltpu.VMEM((2, chips, t, COLS), jnp.float32),
            pltpu.VMEM((2, 2, t, LANES), jnp.float32),
            pltpu.VMEM((2, 2, t, COLS), jnp.float32),
            dma((el,)), dma((2, el)), dma((2,)),
            dma((2,)), dma((2,)), dma((2, 2)), dma((2, 2)), dma((2, 2)), dma((2, 2)),
            reg, reg((2,)), reg((2,)), dma(()),
        ],
        compiler_params=pltpu.CompilerParams(vmem_limit_bytes=VMEM_LIMIT, collective_id=0, has_side_effects=True),
        cost_estimate=pl.CostEstimate(flops=2 * el * n * f * d + 6 * g * n * t * d, bytes_accessed=60_000_000, transcendentals=0),
        name='down',
    )(he, ue2, hit, gr)


def solution(mesh):
    g_ = mesh.shape['ep']
    rows = P(('dp', 'ep'))
    rep = P()

    def local(h0, idx, slot, ln_attn, wq, wk, wv, wo, ln_ffn, ws1, ws3, ws2, ln_moe, wr, ue1, ue3, ue2):
        b, s, d = h0.shape
        top = idx.shape[-1]
        el = ue1.shape[0]
        ne = el * g_
        t = b * s
        cap = CAP_FACTOR * t * top // ne
        u = _rms(h0, ln_moe).reshape(t, d)
        meta = jnp.zeros((16, d), jnp.bfloat16)
        meta = meta.at[0:top, :t].set(idx.reshape(t, top).T.astype(jnp.bfloat16))
        meta = meta.at[8:8 + top, :t].set(slot.reshape(t, top).T.astype(jnp.bfloat16))
        um = jnp.concatenate([u, meta], axis=0)
        ug = lax.all_gather(um, 'ep')
        h = h0.reshape(t, d)
        o = _attention(h, ln_attn, wq, wk, wv)
        dense = _ffn(h, o, ln_ffn, wo, ws1, ws3, ws2)
        me = lax.axis_index('ep')
        base = (me * (el * cap)).astype(jnp.int32).reshape(1)
        p = jnp.arange(g_)
        order = 2 * ((me // 2 + p // 2) % (g_ // 2)) + (me % 2 + p) % 2
        order = order.astype(jnp.int32)
        x, hit, gr = _dispatch(base, order, ug, wr, el, cap, top)
        he = _up(x.reshape(el, g_ * cap, d), ue1, ue3)
        m = _down(he, ue2, hit, gr)
        out = (dense + m).reshape(b, s, d)
        return out.astype(jnp.bfloat16)

    specs = (rows, rows, rows) + (rep,) * 11 + (P('ep'), P('ep'), P('ep'))
    return jax.shard_map(local, mesh=mesh, in_specs=specs, out_specs=rows, check_vma=False)
```

```python
import jax
import jax.numpy as jnp
from jax import lax
from jax.experimental import pallas as pl
from jax.experimental.pallas import tpu as pltpu
from jax.sharding import PartitionSpec as P

HEAD = 128
EPS = 1e-6
CAP_FACTOR = 2


def _rms(x, w):
    xf = x.astype(jnp.float32)
    r = lax.rsqrt(jnp.mean(xf * xf, axis=-1, keepdims=True) + EPS)
    return (xf * r * w.astype(jnp.float32)).astype(jnp.bfloat16)


def _dot(a, b):
    return jnp.dot(a, b, preferred_element_type=jnp.float32)


def _angles(s):
    half = HEAD // 2
    freq = 10000.0 ** (-jnp.arange(half, dtype=jnp.float32) / half)
    ang = jnp.arange(s, dtype=jnp.float32)[:, None] * freq[None, :]
    c, sn = jnp.cos(ang), jnp.sin(ang)
    return jnp.concatenate([c, c], axis=1), jnp.concatenate([-sn, sn], axis=1)


def _attention_kernel(h_ref, ln_ref, cos_ref, sin_ref, wq_ref, wk_ref, wv_ref, o_ref, x_ref):
    s = h_ref.shape[0]
    block = s // 2

    @pl.when(pl.program_id(0) == 0)
    def _():
        x_ref[...] = _rms(h_ref[...], ln_ref[...])

    def rope(z):
        return (z * cos_ref[...] + pltpu.roll(z, HEAD // 2, 1) * sin_ref[...]).astype(jnp.bfloat16)

    q2, k2 = _dot(x_ref[...], wq_ref[...]), _dot(x_ref[...], wk_ref[...])
    v2 = _dot(x_ref[...], wv_ref[...]).astype(jnp.bfloat16)
    for h in range(q2.shape[1] // HEAD):
        cols = slice(h * HEAD, (h + 1) * HEAD)
        q, k, v = rope(q2[:, cols]), rope(k2[:, cols]), v2[:, cols]
        for b in range(2):
            n = (b + 1) * block
            sc = lax.dot_general(q[b * block:n], k[:n], (((1,), (1,)), ((), ())), preferred_element_type=jnp.float32)
            at = lax.broadcasted_iota(jnp.int32, (block, n), 0) + b * block
            sc = jnp.where(at >= lax.broadcasted_iota(jnp.int32, (block, n), 1), sc * HEAD ** -0.5, -1e30)
            e = jnp.exp(sc - jnp.max(sc, axis=1, keepdims=True))
            p = (e * (1.0 / jnp.sum(e, axis=1, keepdims=True))).astype(jnp.bfloat16)
            o_ref[b * block:n, cols] = _dot(p, v[:n]).astype(jnp.bfloat16)


def _attention(h, ln, wq, wk, wv):
    s, d = h.shape
    e = wq.shape[1]
    cos, sin = _angles(s)
    whole = lambda i: (0, 0)
    strip = pl.BlockSpec((d, 2 * HEAD), lambda i: (0, i))
    return pl.pallas_call(
        _attention_kernel,
        grid=(e // (2 * HEAD),),
        in_specs=[pl.BlockSpec((s, d), whole), pl.BlockSpec((1, d), whole), pl.BlockSpec((s, HEAD), whole),
                  pl.BlockSpec((s, HEAD), whole), strip, strip, strip],
        out_specs=pl.BlockSpec((s, 2 * HEAD), lambda i: (0, i)),
        out_shape=jax.ShapeDtypeStruct((s, e), jnp.bfloat16),
        scratch_shapes=[pltpu.VMEM((s, d), jnp.bfloat16)],
        compiler_params=pltpu.CompilerParams(vmem_limit_bytes=VMEM_LIMIT),
        cost_estimate=pl.CostEstimate(flops=6 * s * d * e + 4 * s * s * e, bytes_accessed=6 * d * e, transcendentals=0),
        name='attention',
    )(h, ln.reshape(1, d), cos, sin, wq, wk, wv)


def _ffn_kernel(n1, n2, h_ref, o_ref, ln_ref, wo_ref, w1_ref, w3_ref, w2_ref, out_ref, a_ref, x_ref, s_ref):
    i = pl.program_id(0)

    @pl.when(i < n1)
    def _():
        w = wo_ref.shape[1]
        cols = pl.ds(pl.multiple_of(i * w, w), w)
        a_ref[:, cols] = (h_ref[:, cols].astype(jnp.float32) + _dot(o_ref[...], wo_ref[...])).astype(jnp.bfloat16)

    @pl.when(i == n1)
    def _():
        x_ref[...] = _rms(a_ref[...], ln_ref[...])

    @pl.when(jnp.logical_and(i >= n1, i < n1 + n2))
    def _():
        w = w1_ref.shape[1]
        cols = pl.ds(pl.multiple_of((i - n1) * w, w), w)
        s_ref[:, cols] = (jax.nn.silu(_dot(x_ref[...], w1_ref[...])) * _dot(x_ref[...], w3_ref[...])).astype(jnp.bfloat16)

    @pl.when(i >= n1 + n2)
    def _():
        w = w2_ref.shape[1]
        cols = pl.ds(pl.multiple_of((i - n1 - n2) * w, w), w)
        out_ref[...] = a_ref[:, cols].astype(jnp.float32) + _dot(s_ref[...], w2_ref[...])


def _ffn(h, o, ln, wo, ws1, ws3, ws2):
    s, d = h.shape
    e, f = wo.shape[0], ws1.shape[1]
    c1, c2 = 512, 256
    n1, n2 = d // c1, f // c2
    whole = lambda i: (0, 0)
    clip = lambda x, hi: jnp.minimum(jnp.maximum(x, 0), hi)
    mid = pl.BlockSpec((d, c2), lambda i: (0, clip(i - n1, n2 - 1)))
    return pl.pallas_call(
        lambda *refs: _ffn_kernel(n1, n2, *refs),
        grid=(2 * n1 + n2,),
        in_specs=[pl.BlockSpec((s, d), whole), pl.BlockSpec((s, e), whole), pl.BlockSpec((1, d), whole),
                  pl.BlockSpec((e, c1), lambda i: (0, clip(i, n1 - 1))), mid, mid,
                  pl.BlockSpec((f, c1), lambda i: (0, clip(i - n1 - n2, n1 - 1)))],
        out_specs=pl.BlockSpec((s, c1), lambda i: (0, clip(i - n1 - n2, n1 - 1))),
        out_shape=jax.ShapeDtypeStruct((s, d), jnp.float32),
        scratch_shapes=[pltpu.VMEM((s, d), jnp.bfloat16), pltpu.VMEM((s, d), jnp.bfloat16), pltpu.VMEM((s, f), jnp.bfloat16)],
        compiler_params=pltpu.CompilerParams(vmem_limit_bytes=VMEM_LIMIT),
        cost_estimate=pl.CostEstimate(flops=2 * s * d * e + 6 * s * d * f, bytes_accessed=2 * d * e + 6 * d * f, transcendentals=0),
        name='ffn',
    )(h, o, ln.reshape(1, d), wo, ws1, ws3, ws2)


VMEM_LIMIT = 66_000_000
LANES = 128
COLS = 256
UE = 8
UD = 4
MESH = pl.DeviceIdType.MESH


def _prepare_kernel(h_ref, ln_ref, meta_ref, um_ref):
    t, d = h_ref.shape
    m = meta_ref.shape[0]
    um_ref[:t, :] = _rms(h_ref[...], ln_ref[...])
    um_ref[t:, :] = jnp.zeros((m, d), jnp.bfloat16)
    um_ref[t:, :t] = meta_ref[...]


def _prepare(h, ln, meta):
    t, d = h.shape
    return pl.pallas_call(
        _prepare_kernel,
        out_shape=jax.ShapeDtypeStruct((t + meta.shape[0], d), jnp.bfloat16),
        compiler_params=pltpu.CompilerParams(vmem_limit_bytes=16_000_000),
        cost_estimate=pl.CostEstimate(flops=4 * t * d, bytes_accessed=4 * t * d, transcendentals=0),
        name='prepare',
    )(h, ln.reshape(1, d), meta)


def _dispatch_kernel(el, cap, top, base_ref, order_ref, ug_ref, wr_ref, x_ref, back_ref, gr_ref, hit_ref):
    t = hit_ref.shape[-1]
    ne = wr_ref.shape[-1]
    meta = ug_ref[0, t:t + 16, :t].astype(jnp.float32)
    idx = meta[0:top].astype(jnp.int32)
    row = idx * cap + meta[8:8 + top].astype(jnp.int32) - base_ref[0]
    lg = _dot(ug_ref[0, :t, :], wr_ref[...]).T
    expert = lax.broadcasted_iota(jnp.int32, (ne, t), 0)
    picked = [jnp.sum(jnp.where(expert == idx[j:j + 1], lg, 0.0), axis=0, keepdims=True) for j in range(top)]
    high = picked[0]
    for p in picked[1:]:
        high = jnp.maximum(high, p)
    ex = [jnp.exp(p - high) for p in picked]
    den = ex[0]
    for e in ex[1:]:
        den = den + e
    gate = [e / den for e in ex]
    n = el * cap
    step, wide, blocks = 32, 2 * COLS, 2
    low = lax.broadcasted_iota(jnp.int32, (el, t), 0) * cap
    mine = jnp.full((el, t), -1, jnp.int32)
    scale = jnp.zeros((el, t), jnp.float32)
    for j in range(top):
        inside = jnp.logical_and(row[j:j + 1] >= low, row[j:j + 1] < low + cap)
        mine = jnp.where(inside, row[j:j + 1], mine)
        scale = jnp.where(inside, gate[j], scale)
    col = jnp.concatenate([mine, mine], axis=0).astype(jnp.float32).T.astype(jnp.int32)

    def build(r):
        e = r // cap
        same = lax.broadcasted_iota(jnp.int32, (step, t), 0) + r == mine[e:e + 1]
        hit_ref[r:r + step, :] = jnp.where(same, 1.0, 0.0).astype(jnp.bfloat16)
        g = jnp.sum(jnp.where(same, scale[e:e + 1], 0.0), axis=1, keepdims=True)
        gr_ref[0, r:r + step, :] = jnp.broadcast_to(g, (step, LANES))

    def build_back(r):
        for k in range(0, n, LANES):
            at = lax.broadcasted_iota(jnp.int32, (LANES, LANES), 1) + k
            back = jnp.zeros((LANES, LANES), jnp.float32)
            for e in range(k // cap, (k + LANES - 1) // cap + 1):
                back = jnp.where(at == col[r:r + LANES, e:e + 1], 1.0, back)
            back_ref[0, r:r + LANES, k:k + LANES] = back.astype(jnp.bfloat16)

    part = n // blocks
    for h in range(blocks):
        for r in range(h * part, (h + 1) * part, step):
            build(r)
        for c in range(x_ref.shape[-1] // wide):
            cols = slice(c * wide, (c + 1) * wide)
            x = _dot(hit_ref[h * part:(h + 1) * part], ug_ref[0, :t, cols])
            x_ref[h * part // cap:(h + 1) * part // cap, 0, :, cols] = x.astype(jnp.bfloat16).reshape(part // cap, cap, wide)
    for r in range(0, t, LANES):
        build_back(r)


def _dispatch(base, order, ug, wr, el, cap, top):
    g = order.shape[0]
    _, rows, d = ug.shape
    t = rows - 16
    n = el * cap
    return pl.pallas_call(
        lambda *refs: _dispatch_kernel(el, cap, top, *refs),
        grid_spec=pltpu.PrefetchScalarGridSpec(
            num_scalar_prefetch=2,
            grid=(g,),
            in_specs=[
                pl.BlockSpec((1, rows, d), lambda i, base, order: (order[i], 0, 0)),
                pl.BlockSpec(wr.shape, lambda i, base, order: (0, 0)),
            ],
            out_specs=[
                pl.BlockSpec((el, 1, cap, d), lambda i, base, order: (0, i, 0, 0)),
                pl.BlockSpec((1, t, n), lambda i, base, order: (i, 0, 0)),
                pl.BlockSpec((1, n, LANES), lambda i, base, order: (i, 0, 0)),
            ],
            scratch_shapes=[pltpu.VMEM((n, t), jnp.bfloat16)],
        ),
        out_shape=[
            jax.ShapeDtypeStruct((el, g, cap, d), jnp.bfloat16),
            jax.ShapeDtypeStruct((g, t, n), jnp.bfloat16),
            jax.ShapeDtypeStruct((g, n, LANES), jnp.float32),
        ],
        compiler_params=pltpu.CompilerParams(vmem_limit_bytes=VMEM_LIMIT),
        cost_estimate=pl.CostEstimate(flops=2 * g * n * t * d, bytes_accessed=8_000_000 * g, transcendentals=0),
        name='dispatch',
    )(base, order, ug, wr)


def _up_kernel(x_ref, w1_ref, w3_ref, h_ref):
    for c in range(h_ref.shape[-1] // LANES):
        cols = slice(c * LANES, (c + 1) * LANES)
        r = _dot(x_ref[0], jnp.concatenate([w1_ref[0, :, cols], w3_ref[0, :, cols]], axis=1))
        h_ref[0, :, cols] = (jax.nn.silu(r[:, :LANES]) * r[:, LANES:]).astype(jnp.bfloat16)


def _up(x, ue1, ue3):
    el, n, d = x.shape
    f = ue1.shape[-1]
    return pl.pallas_call(
        _up_kernel,
        grid=(el,),
        in_specs=[
            pl.BlockSpec((1, n, d), lambda i: (i, 0, 0)),
            pl.BlockSpec((1, d, f), lambda i: (i, 0, 0)),
            pl.BlockSpec((1, d, f), lambda i: (i, 0, 0)),
        ],
        out_specs=pl.BlockSpec((1, n, f), lambda i: (i, 0, 0)),
        out_shape=jax.ShapeDtypeStruct((el, n, f), jnp.bfloat16),
        compiler_params=pltpu.CompilerParams(vmem_limit_bytes=VMEM_LIMIT),
        cost_estimate=pl.CostEstimate(flops=4 * el * n * f * d, bytes_accessed=100_000_000, transcendentals=0),
        name='up',
    )(x, ue1, ue3)


def _down_kernel(nc, g, he_hbm, w_hbm, hit_hbm, gr_hbm, dense_hbm, out_ref,
                 he, w, hit, gr, y, p, ra, rb, rf,
                 he_sem, w_sem, in_sem, a_send, a_recv, b_send, b_recv, f_send, f_recv, a_free, b_free, f_free, out_sem, dn, ob, dn_sem):
    el, n, f = he.shape
    t = hit.shape[1]
    cap = n // g
    chips = g // 2
    me = lax.axis_index('ep')
    core, chip = lax.rem(me, 2), lax.div(me, 2)
    mate = me + 1 - 2 * core
    left, right = 2 * lax.rem(chip + chips - 1, chips) + core, 2 * lax.rem(chip + 1, chips) + core
    lchip, rchip, ochip, chip, core = chips - 1, 1, chips // 2, 0, 0

    def he_copy(e):
        return pltpu.make_async_copy(he_hbm.at[e], he.at[e], he_sem.at[e])

    def w_copy(q):
        e, c = lax.rem(q, el), lax.div(q, el)
        cols = pl.ds(pl.multiple_of(c * COLS, COLS), COLS)
        return pltpu.make_async_copy(w_hbm.at[e, :, cols], w.at[lax.rem(c, 2), e], w_sem.at[lax.rem(c, 2), e])

    in_copies = [pltpu.make_async_copy(hit_hbm, hit, in_sem.at[0]), pltpu.make_async_copy(gr_hbm, gr, in_sem.at[1])]

    def a_copy(c):
        return pltpu.make_async_remote_copy(
            src_ref=p.at[lax.rem(c, 3), 1], dst_ref=ra.at[lax.rem(c, 2)],
            send_sem=a_send.at[lax.rem(c, 2)], recv_sem=a_recv.at[lax.rem(c, 2)],
            device_id={'ep': mate}, device_id_type=MESH)

    def b_copy(c, way):
        return pltpu.make_async_remote_copy(
            src_ref=p.at[lax.rem(c, 3), 0, ochip, :, pl.ds(way * LANES, LANES)], dst_ref=rb.at[lax.rem(c, 2), way],
            send_sem=b_send.at[lax.rem(c, 2), way], recv_sem=b_recv.at[lax.rem(c, 2), way],
            device_id={'ep': (left, right)[way]}, device_id_type=MESH)

    def f_copy(c, way):
        return pltpu.make_async_remote_copy(
            src_ref=p.at[lax.rem(c, 3), 0, (lchip, rchip)[way]], dst_ref=rf.at[lax.rem(c, 2), way],
            send_sem=f_send.at[lax.rem(c, 2), way], recv_sem=f_recv.at[lax.rem(c, 2), way],
            device_id={'ep': (left, right)[way]}, device_id_type=MESH)

    def signal(sem, dev):
        pl.semaphore_signal(sem, inc=1, device_id={'ep': dev}, device_id_type=MESH)

    for e in range(el):
        w_copy(e).start()
        he_copy(e).start()
    for copy in in_copies:
        copy.start()

    barrier = pltpu.get_barrier_semaphore()
    for dev in (mate, left, right):
        signal(barrier, dev)
    pl.semaphore_wait(barrier, 3)

    def chunk(i, _):
        q0 = i * el

        @pl.when(i < nc)
        def _():
            @pl.when(i == 0)
            def _():
                for e in range(el):
                    he_copy(e).wait()
                for copy in in_copies:
                    copy.wait()

            @pl.when(i + 1 < nc)
            def _():
                for e in range(el):
                    w_copy(q0 + el + e).start()

            for e in range(el):
                w_copy(q0 + e).wait()

            def expert(e, _):
                q = q0 + e

                yy = jnp.dot(he[e], w[lax.rem(i, 2), e], preferred_element_type=jnp.float32)
                y[:, e] = yy.astype(jnp.bfloat16).reshape(g, cap, COLS)
                return 0

            lax.fori_loop(0, el, expert, 0, unroll=UE)


        @pl.when(jnp.logical_and(i >= 2, i <= nc + 1))
        def _():
            c = i - 2
            s, k = lax.rem(c, 3), lax.rem(c, 2)
            for way in range(2):
                b_copy(c, way).wait_recv()
                b_copy(c, way).wait_send()
            p[s, 0, lchip, :, :LANES] += rb[k, 0]
            p[s, 0, rchip, :, LANES:] += rb[k, 1]

            @pl.when(c < nc - 2)
            def _():
                signal(b_free.at[0], right)
                signal(b_free.at[1], left)

            @pl.when(c >= 2)
            def _():
                pl.semaphore_wait(f_free.at[0], 1)
                pl.semaphore_wait(f_free.at[1], 1)

            f_copy(c, 0).start()
            f_copy(c, 1).start()

        @pl.when(i >= 3)
        def _():
            c = i - 3
            s, k = lax.rem(c, 3), lax.rem(c, 2)
            cols = pl.ds(pl.multiple_of(c * COLS, COLS), COLS)
            base = pltpu.make_async_copy(dense_hbm.at[:, cols], dn, dn_sem)
            base.start()
            f_copy(c, 0).wait_recv()
            f_copy(c, 1).wait_recv()
            base.wait()
            ob[...] = (dn[...] + (p[s, 0, 0] + (rf[k, 0] + rf[k, 1]))).astype(jnp.bfloat16)
            f_copy(c, 0).wait_send()
            f_copy(c, 1).wait_send()
            done = pltpu.make_async_copy(ob, out_ref.at[:, cols], out_sem)
            done.start()
            done.wait()

            @pl.when(c < nc - 2)
            def _():
                signal(f_free.at[0], right)
                signal(f_free.at[1], left)

        @pl.when(i < nc)
        def _():
            s = lax.rem(i, 3)

            def combine(side):
                def dest(dc, _):
                    dd = 2 * dc + side
                    scale = gr[dd]
                    z = y[dd].reshape(n, COLS).astype(jnp.float32) * jnp.concatenate([scale, scale], axis=1)
                    hi = z.astype(jnp.bfloat16)
                    z = z - hi.astype(jnp.float32)
                    mid = z.astype(jnp.bfloat16)
                    lo = (z - mid.astype(jnp.float32)).astype(jnp.bfloat16)
                    r = _dot(hit[dd], jnp.concatenate([hi, mid, lo], axis=1))
                    p[s, side, dc] = r[:, :COLS] + (r[:, COLS:2 * COLS] + r[:, 2 * COLS:])
                    return 0

                lax.fori_loop(0, chips, dest, 0, unroll=UD)

            combine(1)

            @pl.when(i >= 2)
            def _():
                pl.semaphore_wait(a_free, 1)

            a_copy(i).start()
            combine(0)
            cc = a_copy(i)
            cc.wait_recv()
            cc.wait_send()
            k = lax.rem(i, 2)
            p[s, 0, ochip] += ra[k, ochip]
            for r in (0, 1, chips - 1):
                p[s, 0, r] += ra[k, r]

            @pl.when(i < nc - 2)
            def _():
                signal(a_free, mate)

            @pl.when(i >= 2)
            def _():
                pl.semaphore_wait(b_free.at[0], 1)
                pl.semaphore_wait(b_free.at[1], 1)

            b_copy(i, 0).start()
            b_copy(i, 1).start()

        return 0

    lax.fori_loop(0, nc + 3, chunk, 0)


def _down(he, ue2, hit, gr, dense):
    el, n, f = he.shape
    g, t, _ = hit.shape
    d = ue2.shape[-1]
    nc = d // COLS
    chips = g // 2
    dma = pltpu.SemaphoreType.DMA
    reg = pltpu.SemaphoreType.REGULAR
    return pl.pallas_call(
        lambda *refs: _down_kernel(nc, g, *refs),
        in_specs=[pl.BlockSpec(memory_space=pl.ANY)] * 5,
        out_specs=pl.BlockSpec(memory_space=pl.ANY),
        out_shape=jax.ShapeDtypeStruct((t, d), jnp.bfloat16),
        scratch_shapes=[
            pltpu.VMEM((el, n, f), jnp.bfloat16),
            pltpu.VMEM((2, el, f, COLS), jnp.bfloat16),
            pltpu.VMEM((g, t, n), jnp.bfloat16),
            pltpu.VMEM((g, n, LANES), jnp.float32),
            pltpu.VMEM((g, el, n // g, COLS), jnp.bfloat16),
            pltpu.VMEM((3, 2, chips, t, COLS), jnp.float32),
            pltpu.VMEM((2, chips, t, COLS), jnp.float32),
            pltpu.VMEM((2, 2, t, LANES), jnp.float32),
            pltpu.VMEM((2, 2, t, COLS), jnp.float32),
            dma((el,)), dma((2, el)), dma((2,)),
            dma((2,)), dma((2,)), dma((2, 2)), dma((2, 2)), dma((2, 2)), dma((2, 2)),
            reg, reg((2,)), reg((2,)), dma(()),
            pltpu.VMEM((t, COLS), jnp.float32), pltpu.VMEM((t, COLS), jnp.bfloat16), dma(()),
        ],
        compiler_params=pltpu.CompilerParams(vmem_limit_bytes=VMEM_LIMIT, collective_id=0, has_side_effects=True),
        cost_estimate=pl.CostEstimate(flops=2 * el * n * f * d + 6 * g * n * t * d, bytes_accessed=60_000_000, transcendentals=0),
        name='down',
    )(he, ue2, hit, gr, dense)


def solution(mesh):
    g_ = mesh.shape['ep']
    rows = P(('dp', 'ep'))
    rep = P()

    def local(h0, idx, slot, ln_attn, wq, wk, wv, wo, ln_ffn, ws1, ws3, ws2, ln_moe, wr, ue1, ue3, ue2):
        b, s, d = h0.shape
        top = idx.shape[-1]
        el = ue1.shape[0]
        ne = el * g_
        t = b * s
        cap = CAP_FACTOR * t * top // ne
        pad = jnp.zeros((8 - top, t), jnp.bfloat16)
        meta = jnp.concatenate([idx.reshape(t, top).T.astype(jnp.bfloat16), pad,
                                slot.reshape(t, top).T.astype(jnp.bfloat16), pad], axis=0)
        um = _prepare(h0.reshape(t, d), ln_moe, meta)
        ug = lax.all_gather(um, 'ep')
        h = h0.reshape(t, d)
        o = _attention(h, ln_attn, wq, wk, wv)
        dense = _ffn(h, o, ln_ffn, wo, ws1, ws3, ws2)
        me = lax.axis_index('ep')
        base = (me * (el * cap)).astype(jnp.int32).reshape(1)
        p = jnp.arange(g_)
        order = 2 * ((me // 2 + p // 2) % (g_ // 2)) + (me % 2 + p) % 2
        order = order.astype(jnp.int32)
        x, hit, gr = _dispatch(base, order, ug, wr, el, cap, top)
        he = _up(x.reshape(el, g_ * cap, d), ue1, ue3)
        out = _down(he, ue2, hit, gr, dense).reshape(b, s, d)
        return out

    specs = (rows, rows, rows) + (rep,) * 11 + (P('ep'), P('ep'), P('ep'))
    return jax.shard_map(local, mesh=mesh, in_specs=specs, out_specs=rows, check_vma=False)
```
